32 devices in a mesh: slab: 8 (over z, x), gy: 4 (over y, core).
Axes of the slice: x: 2, y: 2, z: 4, core: 2. Of those that a mesh axis runs over, the one named last changes fastest.
Arguments:
- displacement: float32 [3, 32, 64, 512], P(None, None, 'slab', 'gy'), may hold values from -6 to 6
- previous: float32 [3, 32, 64, 512], P(None, None, 'slab', 'gy'), may hold values from -6 to 6
- shear_coef: float32 [32, 64, 512], P(None, 'slab', 'gy'), may hold values from 0.04 to 0.16
- bulk_coef: float32 [32, 64, 512], P(None, 'slab', 'gy'), may hold values from 0.02 to 0.16
- cell_index: int32 [32768], P(('slab', 'gy')), may hold values from 0 to 32767, as said below
- archetype_id: int32 [32768, 1], P(('slab', 'gy')), may hold values from 0 to 1023; in each aligned block of 1024 rows (0 to 1023, 1024 to 2047, ...) at most 2 rows name the same one
- transition: bfloat16 [1024, 256, 256], P(('slab', 'gy')), may hold values from -1 to 1
- forcing: float32 [1024, 3, 256], P(('slab', 'gy')), may hold values from -3 to 3
Outputs:
- final_field: float32 [3, 32, 64, 512], P(None, None, 'slab', 'gy')
- building_state: float32 [32768, 256], P(('slab', 'gy'))
The draws below stay inside these ranges and needn't reach their ends.
Inputs may be any that keep to these rules, and one draw needn't show every extreme that they name: `cell_index`: building b's cell has x between s * 8 and s * 8 + 7, where s = (b // 1024) // 4; y is any. `archetype_id`: among the 1024 buildings of one device no archetype appears more than 2 times.
All inputs are finite; a program needn't handle non-finite values.
Results may differ from the reference program's by a relative error of at most 0.0023.
Values sent between devices are 32-bit elements; how exact they have to be, the bound alone decides.
A program may use at most 64 MiB of HBM per device.

```python
import math
import jax
import jax.numpy as jnp
import numpy as np
from jax import lax

NZ = 32
CX = 8
CY = 128
ARCHETYPES = 1024
STATES = 256
BLD_DEV = 1024
COUPLINGS = 4
EVERY = 5
SUB = 6
NX = 64
NY = 512
BUILDINGS = 32768
CAP = 2
DEVICES = 32


def draw_cell_index(key, part):
    rows = jnp.arange(BUILDINGS, dtype=jnp.int32)
    strip = rows // BLD_DEV // (NY // CY)
    key_x, key_y = jax.random.split(jax.random.fold_in(key, 11))
    along_x = jax.random.randint(key_x, (BUILDINGS,), 0, CX, dtype=jnp.int32)
    along_y = jax.random.randint(key_y, (BUILDINGS,), 0, NY, dtype=jnp.int32)
    return ((strip * CX + along_x) * NY + along_y).astype(jnp.int32)


def draw_transition(key, part):
    key_a, key_b = jax.random.split(jax.random.fold_in(key, 7))
    noise = jax.random.normal(key_a, (ARCHETYPES, STATES, STATES), jnp.float32) * (0.2 / math.sqrt(STATES))
    noise = jnp.clip(noise, -0.25, 0.25)
    diagonal = jax.random.uniform(key_b, (ARCHETYPES, STATES), jnp.float32, 0.4, 0.7)
    matrix = noise + diagonal[:, :, None] * jnp.eye(STATES, dtype=jnp.float32)[None]
    return matrix.astype(jnp.bfloat16)


def block_levels(own_key, dims, cuts, smallest, high):
    def one(dim, blocks):
        heights = jax.random.uniform(jax.random.fold_in(jax.random.fold_in(own_key, 6), dim), (blocks,), jnp.float32, smallest / len(cuts), high / len(cuts))
        return jnp.repeat(jnp.exp(heights), dims[dim] // blocks).reshape((-1,) + (1,) * (len(dims) - dim - 1))

    factor_of = one(*cuts[0])
    for cut in cuts[1:]:
        factor_of = factor_of * one(*cut)
    return factor_of


def deal_out(stream_key, own, number, rows, number_of, top, bound, lean):
    sequence = jax.random.permutation(stream_key, number_of)
    crowded, ordinary = load_shares(number_of, rows * top, bound, lean, True), load_shares(number_of, rows * top, bound, lean, False)
    places = jnp.arange(number_of)

    def named(tallies, rotation):
        used = int((tallies > 0).sum())
        fixed = max(1, used // 4)
        moved = fixed + (places - fixed + rotation * (used - fixed)) % max(1, number_of - fixed)
        return jnp.zeros((number_of,), jnp.int32).at[sequence[jnp.where(places < fixed, places, moved)]].set(jnp.asarray(tallies, jnp.int32))

    tallies = jnp.where(number % 4 == 0, named(crowded, number // 4), named(ordinary, number - number // 4 - 1))
    mixed = jax.random.permutation(jax.random.fold_in(own, 3), number_of)
    giver, sink = mixed[0:number_of // 2 * 2:2], mixed[1:number_of // 2 * 2:2]
    room = jnp.minimum(tallies[giver] - 1, bound - tallies[sink]) // 2
    room = jnp.where((giver == sequence[0]) | (sink == sequence[0]) | (tallies[sink] == 0), 0, jnp.maximum(room, 0))
    moved = jax.random.randint(jax.random.fold_in(own, 4), (number_of // 2,), 0, 1 << 20) % (room + 1)
    tallies = tallies.at[giver].add(-moved).at[sink].add(moved)
    items = jnp.searchsorted(jnp.cumsum(tallies), jnp.arange(rows * top), side="right").astype(jnp.int32)
    table = items.reshape(top, rows).T
    table = table[jax.random.permutation(jax.random.fold_in(own, 1), rows)]
    rotation = jax.random.randint(jax.random.fold_in(own, 2), (rows, 1), 0, top)
    return jnp.take_along_axis(table, (jnp.arange(top)[None, :] + rotation) % top, axis=1)


def load_shares(count, total, bound, lean, full):
    portions = [(1 << 20) // math.isqrt(rank ** lean) + 1 for rank in range(1, count + 1)]
    largest = bound if full else min(bound, max(-(-total // count), total * portions[0] // sum(portions)))
    least = 1 if total - largest >= count - 1 else 0
    holding, surplus = [largest] + [least] * (count - 1), total - largest - least * (count - 1)
    while surplus > 0:
        movable = [i for i in range(1, count) if holding[i] < largest] or [i for i in range(1, count) if holding[i] < bound]
        mass, left = sum([portions[i] for i in movable]), surplus
        for i in movable:
            extra = min(bound - holding[i], max(1, left * portions[i] // mass), surplus)
            holding[i] = holding[i] + extra
            surplus = surplus - extra
    return np.array(holding)


def centred(rng, shape, width, bound, cuts=(), held_as=jnp.bfloat16):
    array = jax.random.normal(rng, shape, jnp.float32) * width
    if len(cuts) > 0:
        array = block_levels(rng, shape, cuts, -0.22, 0.18) * array
    return jnp.clip(array, min=-bound, max=bound).astype(held_as)


def setup_inputs(seed: int = 0) -> dict:
    streams_of = jax.random.split(jax.random.key(seed), 9)
    displacement = centred(streams_of[0], (3, NZ, NX, NY), 1.0, 6.0, ((2, 8), (3, 4)), jnp.float32)
    previous = centred(streams_of[1], (3, NZ, NX, NY), 1.0, 6.0, ((2, 8), (3, 4)), jnp.float32)
    shear_coef = jnp.clip(jnp.exp(math.log(0.16) - 1.3862944 * jax.random.uniform(streams_of[2], (NZ, NX, NY), jnp.float32) ** block_levels(streams_of[2], (NZ, NX, NY), ((1, 8), (2, 4)), -0.2, 0.2)), 0.04, 0.16)
    bulk_coef = jnp.clip(jnp.exp(math.log(0.16) - 2.0794415 * jax.random.uniform(streams_of[3], (NZ, NX, NY), jnp.float32) ** block_levels(streams_of[3], (NZ, NX, NY), ((1, 8), (2, 4)), -0.2, 0.2)), 0.02, 0.16)
    cell_index = draw_cell_index(jax.random.fold_in(streams_of[8], 71), 0)
    archetype_id_keys = jax.random.split(jax.random.fold_in(streams_of[5], 1), BUILDINGS // BLD_DEV)
    archetype_id_turns = jax.random.permutation(jax.random.fold_in(streams_of[5], 3), BUILDINGS // BLD_DEV)
    archetype_id = jax.vmap(lambda own, number: deal_out(jax.random.fold_in(streams_of[5], 2), own, number, BLD_DEV, ARCHETYPES, 1, CAP, 2))(archetype_id_keys, archetype_id_turns).reshape((BUILDINGS, 1))
    transition = draw_transition(jax.random.fold_in(streams_of[8], 71), 0)
    forcing = centred(streams_of[7], (ARCHETYPES, 3, STATES), 0.5, 3.0, ((0, 32),), jnp.float32)
    return dict(displacement=displacement, previous=previous, shear_coef=shear_coef, bulk_coef=bulk_coef, cell_index=cell_index, archetype_id=archetype_id, transition=transition, forcing=forcing)


FIRST = ((-2, 1.0 / 12.0), (-1, -8.0 / 12.0), (1, 8.0 / 12.0), (2, -1.0 / 12.0))
SECOND = ((-2, -1.0 / 12.0), (-1, 16.0 / 12.0), (0, -30.0 / 12.0), (1, 16.0 / 12.0), (2, -1.0 / 12.0))
COMPONENT_AXIS = (1, 2, 0)


def pad_depth(padded):
    extent = padded.shape
    below = jnp.zeros((extent[0], 2, extent[2], extent[3]), padded.dtype)
    return jnp.concatenate([padded[:, 2:0:-1], padded, below], axis=1)


def shifted(volume, offsets):
    starts = [2 + offsets[0], 2 + offsets[1], 2 + offsets[2]]
    return volume[starts[0]:starts[0] + volume.shape[0] - 4,
                  starts[1]:starts[1] + volume.shape[1] - 4,
                  starts[2]:starts[2] + volume.shape[2] - 4]


def second_along(volume, main_axis):
    summed = None
    for amount, weight in SECOND:
        offsets = [0, 0, 0]
        offsets[main_axis] = amount
        term = weight * shifted(volume, offsets)
        summed = term if summed is None else summed + term
    return summed


def mixed_along(volume, main_axis, other_axis):
    summed = None
    for amount_a, weight_a in FIRST:
        for amount_b, weight_b in FIRST:
            offsets = [0, 0, 0]
            offsets[main_axis] = amount_a
            offsets[other_axis] = amount_b
            term = (weight_a * weight_b) * shifted(volume, offsets)
            summed = term if summed is None else summed + term
    return summed


def accelerate(padded, shear_coef, bulk_coef):
    results = []
    for component in range(3):
        volume = padded[component]
        main_axis = COMPONENT_AXIS[component]
        seconds = [second_along(volume, axis_a) for axis_a in range(3)]
        laplacian = seconds[0] + seconds[1] + seconds[2]
        divergence = seconds[main_axis]
        for partner in range(3):
            if partner != component:
                divergence = divergence + mixed_along(padded[partner], main_axis, COMPONENT_AXIS[partner])
        results.append(shear_coef * laplacian + bulk_coef * divergence)
    return jnp.stack(results)


def advance_grid(field, former, shear_coef, bulk_coef):
    padded = pad_depth(jnp.pad(field, ((0, 0), (0, 0), (2, 2), (2, 2))))
    return 2.0 * field - former + accelerate(padded, shear_coef, bulk_coef)


def ranks_of(members):
    order = jnp.arange(members.shape[0], dtype=jnp.int32)
    earlier = (members[:, None] == members[None, :]) & (order[None, :] < order[:, None])
    return jnp.sum(earlier.astype(jnp.int32), axis=1).astype(jnp.int32)


def reference(displacement, previous, shear_coef, bulk_coef, cell_index, archetype_id, transition, forcing):
    kinds = archetype_id[:, 0].astype(jnp.int32)
    position = lax.map(ranks_of, kinds.reshape(DEVICES, BLD_DEV)).reshape(-1).astype(jnp.int32)
    home_dev = (jnp.arange(BUILDINGS, dtype=jnp.int32) // BLD_DEV).astype(jnp.int32)
    states = jnp.zeros((BUILDINGS, STATES), jnp.float32)
    matrices = transition.astype(jnp.float32)
    field, former = displacement, previous
    for moment in range(COUPLINGS):
        for inner in range(EVERY):
            field, former = advance_grid(field, former, shear_coef, bulk_coef), field
        surface = field[:, 0].reshape(3, NX * NY)
        ground = jnp.take(surface, cell_index, axis=1)
        slots = jnp.zeros((ARCHETYPES, DEVICES, CAP, STATES), jnp.float32).at[kinds, home_dev, position].set(states)
        motion = jnp.zeros((ARCHETYPES, 3, DEVICES, CAP), jnp.float32).at[kinds, :, home_dev, position].set(ground.T)
        drive = motion[:, 0, :, :, None] * forcing[:, 0, None, None, :]
        drive = drive + motion[:, 1, :, :, None] * forcing[:, 1, None, None, :]
        drive = drive + motion[:, 2, :, :, None] * forcing[:, 2, None, None, :]
        for inner in range(SUB):
            rounded = lax.optimization_barrier(slots.astype(jnp.bfloat16)).astype(jnp.float32)
            slots = jnp.einsum("adck,ajk->adcj", rounded, matrices) + drive
        states = slots[kinds, home_dev, position]
    return field, states
```

```python
import functools

import jax
import jax.numpy as jnp
from jax import lax
from jax.experimental import pallas as pl
from jax.experimental.pallas import tpu as pltpu
from jax.sharding import PartitionSpec as P

COUPLINGS = 4
EVERY = 5
SUB = 6
CAP = 2
CHUNKS = 2
ARCH_BLOCK = 4
PLANES = 4

A0, A1, A2 = -30.0 / 12.0, 16.0 / 12.0, -1.0 / 12.0
B1, B2 = 8.0 / 12.0, -1.0 / 12.0
DIRECTIONS = ((-1, 0), (1, 0), (0, -1), (0, 1), (-1, -1), (1, -1), (-1, 1), (1, 1))


def second(mid, plus1, minus1, plus2, minus2):
    return A0 * mid + A1 * (plus1 + minus1) + A2 * (plus2 + minus2)


def first(plus1, minus1, plus2, minus2):
    return B1 * (plus1 - minus1) + B2 * (plus2 - minus2)


def grid_kernel(
    steps, every, d_ref, p_ref, sh_ref, bk_ref, f_ref, surf_ref,
    buf, ps, pr, ht, ah, hx, e_ref, s_ref, send, recv,
):
    nz, cx, cy = sh_ref.shape
    slab, gy = lax.axis_index("slab"), lax.axis_index("gy")
    slabs, gys = lax.axis_size("slab"), lax.axis_size("gy")
    blocks = nz // PLANES

    def exists(dx, dy):
        x, y = slab + dx, gy + dy
        return (x >= 0) & (x < slabs) & (y >= 0) & (y < gys)

    buf[...] = jnp.zeros_like(buf)
    pr[...] = jnp.zeros_like(pr)
    ht[...] = jnp.zeros_like(ht)
    e_ref[...] = jnp.zeros_like(e_ref)
    buf[0, :, 2 : nz + 2, 8:16, :] = d_ref[...]
    buf[1, :, 2 : nz + 2, 8:16, :] = p_ref[...]

    barrier = pltpu.get_barrier_semaphore()
    for dx, dy in DIRECTIONS:
        @pl.when(exists(dx, dy))
        def _():
            pl.semaphore_signal(
                barrier, inc=1, device_id=(slab + dx, gy + dy),
                device_id_type=pl.DeviceIdType.MESH,
            )
    spans = [
        1 + jnp.where(at > 0, 1, 0) + jnp.where(at < size - 1, 1, 0)
        for at, size in ((slab, slabs), (gy, gys))
    ]
    pl.semaphore_wait(barrier, spans[0] * spans[1] - 1)

    def copy_of(k, par):
        dx, dy = DIRECTIONS[k]
        mine = slice(0, 2) if dx < 0 else slice(cx - 2, cx)
        theirs = slice(16, 18) if dx < 0 else slice(6, 8)
        if dy == 0:
            src = buf.at[par, :, 2 : nz + 2, mine.start + 8 : mine.stop + 8, :]
            dst = buf.at[par, :, 2 : nz + 2, theirs, :]
        elif dx == 0:
            src = ps.at[par]
            dst = pr.at[par, 1 if dy < 0 else 0, :, 8:16, :]
        else:
            src = ps.at[par, :, mine, :]
            dst = pr.at[par, 1 if dy < 0 else 0, :, theirs, :]
        return pltpu.make_async_remote_copy(
            src_ref=src, dst_ref=dst, send_sem=send.at[par, k], recv_sem=recv.at[par, k],
            device_id=(slab + dx, gy + dy), device_id_type=pl.DeviceIdType.MESH,
        )

    lane3 = lax.broadcasted_iota(jnp.int32, (PLANES, cx, cy), 2)
    lane = lax.broadcasted_iota(jnp.int32, (cx, cy), 1)
    row3 = lax.broadcasted_iota(jnp.int32, (PLANES, cx, cy), 1)
    row = lax.broadcasted_iota(jnp.int32, (cx, cy), 0)

    def along_y(core, halo):
        return (
            pltpu.roll(jnp.where(lane3 < 1, halo, core), cy - 1, 2),
            pltpu.roll(jnp.where(lane3 >= cy - 1, halo, core), 1, 2),
            pltpu.roll(jnp.where(lane3 < 2, halo, core), cy - 2, 2),
            pltpu.roll(jnp.where(lane3 >= cy - 2, halo, core), 2, 2),
        )

    def step(n, carry):
        par = lax.rem(n, 2)
        new = 1 - par

        for k in range(2):
            @pl.when(exists(*DIRECTIONS[k]))
            def _():
                copy_of(k, par).start()

        for c in range(3):
            packed = jnp.zeros((cx, cy), jnp.float32)
            for d in range(nz):
                turned = pltpu.roll(buf[par, c, d + 2, 8:16, :], 2 + 4 * d, 1) if (2 + 4 * d) % cy else buf[par, c, d + 2, 8:16, :]
                packed = jnp.where((lane >= 4 * d) & (lane < 4 * d + 4), turned, packed)
            ps[par, c] = packed

        for k in range(2, 8):
            @pl.when(exists(*DIRECTIONS[k]))
            def _():
                copy_of(k, par).start()

        for c in range(3):
            buf[par, c, 0, 8:16, :] = buf[par, c, 4, 8:16, :]
            buf[par, c, 1, 8:16, :] = buf[par, c, 3, 8:16, :]

        for k in range(8):
            @pl.when(exists(*DIRECTIONS[k]))
            def _():
                copy_of(k, par).wait_send()
        for k in range(8):
            dx, dy = DIRECTIONS[k]
            @pl.when(exists(-dx, -dy))
            def _():
                copy_of(k, par).wait_recv()

        for lo in (0, 16):
            buf[par, 2, 0, lo : lo + 8, :] = buf[par, 2, 4, lo : lo + 8, :]
            buf[par, 2, 1, lo : lo + 8, :] = buf[par, 2, 3, lo : lo + 8, :]

        from_left = lax.rem(lane, 4) < 2

        def joined(c, lo):
            return jnp.where(from_left, pr[par, 0, c, lo : lo + 8, :], pr[par, 1, c, lo : lo + 8, :])

        g = [joined(c, 8) for c in range(3)]
        g_y = jnp.where(row < 4, joined(1, 16), joined(1, 0))
        g_x = jnp.where(row < 4, joined(0, 16), joined(0, 0))
        a_g = first(
            pltpu.roll(jnp.where(row < 1, g_x, g[0]), cx - 1, 0),
            pltpu.roll(jnp.where(row >= cx - 1, g_x, g[0]), 1, 0),
            pltpu.roll(jnp.where(row < 2, g_x, g[0]), cx - 2, 0),
            pltpu.roll(jnp.where(row >= cx - 2, g_x, g[0]), 2, 0),
        )
        for d in range(nz):
            back = (cy - 4 * d - 2) % cy
            for c in range(3):
                ht[c, d + 2] = pltpu.roll(g[c], back, 1)
            ah[d] = pltpu.roll(a_g, back, 1)
            hx[d] = pltpu.roll(g_y, back, 1)
        ht[2, 0] = ht[2, 4]
        ht[2, 1] = ht[2, 3]

        def u(c, d, shift, lo):
            return buf[par, c, pl.ds(d + 2 + shift, PLANES), lo : lo + 8, :]

        def prepare(b, carry):
            d = b * PLANES
            a = first(u(0, d, 0, 9), u(0, d, 0, 7), u(0, d, 0, 10), u(0, d, 0, 6))
            bb = first(*along_y(u(1, d, 0, 8), ht[1, pl.ds(d + 2, PLANES)]))
            e_ref[pl.ds(d + 2, PLANES)] = a + bb
            cc = first(u(2, d, 1, 8), u(2, d, -1, 8), u(2, d, 2, 8), u(2, d, -2, 8))
            s_ref[pl.ds(d, PLANES), 8:16, :] = bb + cc

            def mixed(comp, shift):
                return jnp.where(row3 < 4, u(comp, d, shift, 16), u(comp, d, shift, 0))

            s_halo = first(*along_y(mixed(1, 0), hx[pl.ds(d, PLANES)])) + first(
                mixed(2, 1), mixed(2, -1), mixed(2, 2), mixed(2, -2)
            )
            s_ref[pl.ds(d, PLANES), 0:8, :] = s_halo
            s_ref[pl.ds(d, PLANES), 16:24, :] = s_halo
            return carry

        lax.fori_loop(0, blocks, prepare, 0)
        e_ref[0] = e_ref[4]
        e_ref[1] = e_ref[3]

        def advance(b, carry):
            d = b * PLANES
            sh = sh_ref[pl.ds(d, PLANES)]
            bk = bk_ref[pl.ds(d, PLANES)]

            def h(c, shift):
                return ht[c, pl.ds(d + 2 + shift, PLANES)]

            def s(lo):
                return s_ref[pl.ds(d, PLANES), lo : lo + 8, :]

            def e(shift):
                return e_ref[pl.ds(d + 2 + shift, PLANES)]

            a = first(u(0, d, 0, 9), u(0, d, 0, 7), u(0, d, 0, 10), u(0, d, 0, 6))
            cc = first(u(2, d, 1, 8), u(2, d, -1, 8), u(2, d, 2, 8), u(2, d, -2, 8))
            c_halo = first(h(2, 1), h(2, -1), h(2, 2), h(2, -2))
            t_halo = ah[pl.ds(d, PLANES)] + c_halo
            for c in range(3):
                mid = u(c, d, 0, 8)
                along = (
                    second(mid, u(c, d, 0, 9), u(c, d, 0, 7), u(c, d, 0, 10), u(c, d, 0, 6)),
                    second(mid, *along_y(mid, h(c, 0))),
                    second(mid, u(c, d, 1, 8), u(c, d, -1, 8), u(c, d, 2, 8), u(c, d, -2, 8)),
                )
                if c == 0:
                    cross = first(s(9), s(7), s(10), s(6))
                elif c == 1:
                    cross = first(*along_y(a + cc, t_halo))
                else:
                    cross = first(e(1), e(-1), e(2), e(-2))
                acc = sh * (along[0] + along[1] + along[2]) + bk * (along[c] + cross)
                place = (new, c, pl.ds(d + 2, PLANES), slice(8, 16), slice(None))
                buf[place] = 2.0 * mid - buf[place] + acc
            return carry

        lax.fori_loop(0, blocks, advance, 0)
        surf_ref[lax.div(n, every)] = buf[new, :, 2, 8:16, :]
        return carry

    lax.fori_loop(0, steps, step, 0)
    f_ref[...] = buf[steps % 2, :, 2 : nz + 2, 8:16, :]


def run_grid(displacement, previous, shear_coef, bulk_coef):
    _, nz, cx, cy = displacement.shape
    vmem = pl.BlockSpec(memory_space=pltpu.VMEM)
    f32 = jnp.float32
    return pl.pallas_call(
        functools.partial(grid_kernel, COUPLINGS * EVERY, EVERY),
        out_shape=(
            jax.ShapeDtypeStruct(displacement.shape, f32),
            jax.ShapeDtypeStruct((COUPLINGS, 3, cx, cy), f32),
        ),
        in_specs=[vmem] * 4,
        out_specs=(vmem, vmem),
        scratch_shapes=[
            pltpu.VMEM((2, 3, nz + 4, cx + 16, cy), f32),
            pltpu.VMEM((2, 3, cx, cy), f32),
            pltpu.VMEM((2, 2, 3, cx + 16, cy), f32),
            pltpu.VMEM((3, nz + 4, cx, cy), f32),
            pltpu.VMEM((nz, cx, cy), f32),
            pltpu.VMEM((nz, cx, cy), f32),
            pltpu.VMEM((nz + 4, cx, cy), f32),
            pltpu.VMEM((nz, cx + 16, cy), f32),
            pltpu.SemaphoreType.DMA((2, 8)),
            pltpu.SemaphoreType.DMA((2, 8)),
        ],
        compiler_params=pltpu.CompilerParams(
            collective_id=0, has_side_effects=True, vmem_limit_bytes=32 * 1024 * 1024
        ),
    )(displacement, previous, shear_coef, bulk_coef)


def building_kernel(couplings, sub, m_ref, f_ref, t_ref, o_ref):
    block, rows, _ = m_ref.shape
    width = t_ref.shape[1]
    states = [jnp.zeros((rows, width), jnp.float32) for _ in range(block)]
    for moment in range(couplings):
        drives = []
        for i in range(block):
            drive = m_ref[i, :, 3 * moment : 3 * moment + 1] * f_ref[i, 0:1, :]
            drive = drive + m_ref[i, :, 3 * moment + 1 : 3 * moment + 2] * f_ref[i, 1:2, :]
            drive = drive + m_ref[i, :, 3 * moment + 2 : 3 * moment + 3] * f_ref[i, 2:3, :]
            drives.append(drive)
        for inner in range(sub):
            for i in range(block):
                if moment == 0 and inner == 0:
                    states[i] = drives[i]
                else:
                    states[i] = drives[i] + lax.dot_general(
                        states[i].astype(jnp.bfloat16), t_ref[i],
                        (((1,), (1,)), ((), ())), preferred_element_type=jnp.float32,
                    )
    for i in range(block):
        o_ref[:, CAP * i : CAP * (i + 1), :] = states[i].reshape(rows // CAP, CAP, width)


def run_buildings(motion, forcing, transition, start, kinds):
    rows, parts = motion.shape[1], motion.shape[2]
    width = transition.shape[1]
    first_block = start // ARCH_BLOCK
    return pl.pallas_call(
        functools.partial(building_kernel, COUPLINGS, SUB),
        grid=(kinds // ARCH_BLOCK,),
        out_shape=jax.ShapeDtypeStruct((rows // CAP, kinds * CAP, width), jnp.float32),
        in_specs=[
            pl.BlockSpec((ARCH_BLOCK, rows, parts), lambda i: (i + first_block, 0, 0)),
            pl.BlockSpec((ARCH_BLOCK, 3, width), lambda i: (i + first_block, 0, 0)),
            pl.BlockSpec((ARCH_BLOCK, width, width), lambda i: (i + first_block, 0, 0)),
        ],
        out_specs=pl.BlockSpec((rows // CAP, ARCH_BLOCK * CAP, width), lambda i: (0, i, 0)),
        cost_estimate=pl.CostEstimate(
            flops=2 * kinds * rows * width * width * COUPLINGS * SUB,
            bytes_accessed=2 * kinds * width * width + 4 * kinds * rows * width,
            transcendentals=0,
        ),
    )(motion, forcing, transition)


def per_device(
    displacement, previous, shear_coef, bulk_coef, cell_index, archetype_id, transition, forcing
):
    groups = lax.axis_size("slab") * lax.axis_size("gy")
    arch_local = transition.shape[0]
    width = transition.shape[1]
    slots_dev = arch_local * CAP
    count = cell_index.shape[0]
    kinds = archetype_id[:, 0]
    order = jnp.arange(count, dtype=jnp.int32)
    earlier = (kinds[:, None] == kinds[None, :]) & (order[None, :] < order[:, None])
    position = jnp.sum(earlier.astype(jnp.int32), axis=1)
    slot_index = kinds * CAP + position
    cells = displacement.shape[2] * displacement.shape[3] * lax.axis_size("gy")
    local_cell = cell_index - lax.axis_index("slab") * cells
    slots = jnp.arange(groups * slots_dev, dtype=jnp.int32)
    slot_cell = jnp.sum(
        jnp.where(slot_index[None, :] == slots[:, None], local_cell[None, :], 0), axis=1
    )

    field, surface = run_grid(displacement, previous, shear_coef, bulk_coef)

    parts = 3 * COUPLINGS
    surface = lax.all_gather(surface, "gy", axis=3, tiled=True)
    table = surface.reshape(parts, cells).T
    motion = jnp.take(table, slot_cell, axis=0, mode="clip")
    motion = motion.reshape(groups, slots_dev, parts).transpose(0, 2, 1)
    pushed = lax.all_to_all(motion, ("slab", "gy"), split_axis=0, concat_axis=0, tiled=True)
    pushed = pushed.reshape(groups, parts, arch_local, CAP).transpose(2, 0, 3, 1)
    pushed = pushed.reshape(arch_local, groups * CAP, parts)

    share = arch_local // CHUNKS
    pieces = []
    for chunk in range(CHUNKS):
        states = run_buildings(pushed, forcing, transition, chunk * share, share)
        returned = lax.all_to_all(
            states, ("slab", "gy"), split_axis=0, concat_axis=0, tiled=True
        )
        pieces.append(returned.reshape(groups * share * CAP, width))
    owner, kind = kinds // arch_local, kinds % arch_local
    chunk_of = kind // share
    home = chunk_of * (groups * share * CAP) + owner * (share * CAP)
    home = home + (kind - chunk_of * share) * CAP + position
    home_state = jnp.take(jnp.concatenate(pieces, axis=0), home, axis=0, mode="clip")
    return (field, home_state)


def solution(mesh):
    in_specs = (
        P(None, None, "slab", "gy"),
        P(None, None, "slab", "gy"),
        P(None, "slab", "gy"),
        P(None, "slab", "gy"),
        P(("slab", "gy")),
        P(("slab", "gy"), None),
        P(("slab", "gy"), None, None),
        P(("slab", "gy"), None, None),
    )
    out_specs = (P(None, None, "slab", "gy"), P(("slab", "gy"), None))
    return jax.shard_map(
        per_device, mesh=mesh, in_specs=in_specs, out_specs=out_specs, check_vma=False
    )
```

```python
import functools

import jax
import jax.numpy as jnp
from jax import lax
from jax.experimental import pallas as pl
from jax.experimental.pallas import tpu as pltpu
from jax.sharding import PartitionSpec as P

COUPLINGS = 4
EVERY = 5
SUB = 6
CAP = 2
CHUNKS = 2
ARCH_BLOCK = 4
PLANES = 4

A0, A1, A2 = -30.0 / 12.0, 16.0 / 12.0, -1.0 / 12.0
B1, B2 = 8.0 / 12.0, -1.0 / 12.0
DIRECTIONS = ((-1, 0), (1, 0), (0, -1), (0, 1), (-1, -1), (1, -1), (-1, 1), (1, 1))


def second(mid, plus1, minus1, plus2, minus2):
    return A0 * mid + A1 * (plus1 + minus1) + A2 * (plus2 + minus2)


def first(plus1, minus1, plus2, minus2):
    return B1 * (plus1 - minus1) + B2 * (plus2 - minus2)


def grid_kernel(
    steps, every, d_ref, p_ref, sh_ref, bk_ref, f_ref, surf_ref,
    buf, ps, pr, ht, ah, hx, e_ref, s_ref, bb_ref, cc_ref, send, recv,
):
    nz, cx, cy = sh_ref.shape
    slab, gy = lax.axis_index("slab"), lax.axis_index("gy")
    slabs, gys = lax.axis_size("slab"), lax.axis_size("gy")
    blocks = nz // PLANES

    def exists(dx, dy):
        x, y = slab + dx, gy + dy
        return (x >= 0) & (x < slabs) & (y >= 0) & (y < gys)

    buf[...] = jnp.zeros_like(buf)
    pr[...] = jnp.zeros_like(pr)
    ht[...] = jnp.zeros_like(ht)
    e_ref[...] = jnp.zeros_like(e_ref)
    buf[0, :, 2 : nz + 2, 8:16, :] = d_ref[...]
    buf[1, :, 2 : nz + 2, 8:16, :] = p_ref[...]

    barrier = pltpu.get_barrier_semaphore()
    for dx, dy in DIRECTIONS:
        @pl.when(exists(dx, dy))
        def _():
            pl.semaphore_signal(
                barrier, inc=1, device_id=(slab + dx, gy + dy),
                device_id_type=pl.DeviceIdType.MESH,
            )
    spans = [
        1 + jnp.where(at > 0, 1, 0) + jnp.where(at < size - 1, 1, 0)
        for at, size in ((slab, slabs), (gy, gys))
    ]
    pl.semaphore_wait(barrier, spans[0] * spans[1] - 1)

    def copy_of(k, par):
        dx, dy = DIRECTIONS[k]
        mine = slice(0, 2) if dx < 0 else slice(cx - 2, cx)
        theirs = slice(16, 18) if dx < 0 else slice(6, 8)
        if dy == 0:
            src = buf.at[par, :, 2 : nz + 2, mine.start + 8 : mine.stop + 8, :]
            dst = buf.at[par, :, 2 : nz + 2, theirs, :]
        elif dx == 0:
            src = ps.at[par]
            dst = pr.at[par, 1 if dy < 0 else 0, :, 8:16, :]
        else:
            src = ps.at[par, :, mine, :]
            dst = pr.at[par, 1 if dy < 0 else 0, :, theirs, :]
        return pltpu.make_async_remote_copy(
            src_ref=src, dst_ref=dst, send_sem=send.at[par, k], recv_sem=recv.at[par, k],
            device_id=(slab + dx, gy + dy), device_id_type=pl.DeviceIdType.MESH,
        )

    lane3 = lax.broadcasted_iota(jnp.int32, (PLANES, cx, cy), 2)
    lane = lax.broadcasted_iota(jnp.int32, (cx, cy), 1)
    row3 = lax.broadcasted_iota(jnp.int32, (PLANES, cx, cy), 1)
    row = lax.broadcasted_iota(jnp.int32, (cx, cy), 0)

    def along_y(core, halo):
        return (
            pltpu.roll(jnp.where(lane3 < 1, halo, core), cy - 1, 2),
            pltpu.roll(jnp.where(lane3 >= cy - 1, halo, core), 1, 2),
            pltpu.roll(jnp.where(lane3 < 2, halo, core), cy - 2, 2),
            pltpu.roll(jnp.where(lane3 >= cy - 2, halo, core), 2, 2),
        )

    def step(n, carry):
        par = lax.rem(n, 2)
        new = 1 - par

        for k in range(2):
            @pl.when(exists(*DIRECTIONS[k]))
            def _():
                copy_of(k, par).start()

        for c in range(3):
            packed = jnp.zeros((cx, cy), jnp.float32)
            for d in range(nz):
                turned = pltpu.roll(buf[par, c, d + 2, 8:16, :], 2 + 4 * d, 1) if (2 + 4 * d) % cy else buf[par, c, d + 2, 8:16, :]
                packed = jnp.where((lane >= 4 * d) & (lane < 4 * d + 4), turned, packed)
            ps[par, c] = packed

        for k in range(2, 8):
            @pl.when(exists(*DIRECTIONS[k]))
            def _():
                copy_of(k, par).start()

        for c in range(3):
            buf[par, c, 0, 8:16, :] = buf[par, c, 4, 8:16, :]
            buf[par, c, 1, 8:16, :] = buf[par, c, 3, 8:16, :]

        def u(c, d, shift, lo):
            return buf[par, c, pl.ds(d + 2 + shift, PLANES), lo : lo + 8, :]

        def core(c, d):
            return (new, c, pl.ds(d + 2, PLANES), slice(8, 16), slice(None))

        def local(b, carry):
            d = b * PLANES
            sh = sh_ref[pl.ds(d, PLANES)]
            bk = bk_ref[pl.ds(d, PLANES)]
            for c in range(3):
                mid = u(c, d, 0, 8)
                near = (u(c, d, 1, 8), u(c, d, -1, 8), u(c, d, 2, 8), u(c, d, -2, 8))
                coef = sh + bk if c == 2 else sh
                buf[core(c, d)] = 2.0 * mid - buf[core(c, d)] + coef * second(mid, *near)
                if c == 2:
                    cc_ref[pl.ds(d, PLANES)] = first(*near)
            return carry

        lax.fori_loop(0, blocks, local, 0)

        def await_halos(ks):
            for k in ks:
                dx, dy = DIRECTIONS[k]
                @pl.when(exists(-dx, -dy))
                def _():
                    copy_of(k, par).wait_recv()

        await_halos(range(2, 8))

        from_left = lax.rem(lane, 4) < 2

        def joined(c, lo):
            return jnp.where(from_left, pr[par, 0, c, lo : lo + 8, :], pr[par, 1, c, lo : lo + 8, :])

        g = [joined(c, 8) for c in range(3)]
        g_y = jnp.where(row < 4, joined(1, 16), joined(1, 0))
        g_x = jnp.where(row < 4, joined(0, 16), joined(0, 0))
        a_g = first(
            pltpu.roll(jnp.where(row < 1, g_x, g[0]), cx - 1, 0),
            pltpu.roll(jnp.where(row >= cx - 1, g_x, g[0]), 1, 0),
            pltpu.roll(jnp.where(row < 2, g_x, g[0]), cx - 2, 0),
            pltpu.roll(jnp.where(row >= cx - 2, g_x, g[0]), 2, 0),
        )
        for d in range(nz):
            back = (cy - 4 * d - 2) % cy
            for c in range(3):
                ht[c, d + 2] = pltpu.roll(g[c], back, 1)
            ah[d] = pltpu.roll(a_g, back, 1)
            hx[d] = pltpu.roll(g_y, back, 1)
        ht[2, 0] = ht[2, 4]
        ht[2, 1] = ht[2, 3]

        def sideways(b, carry):
            d = b * PLANES
            sh = sh_ref[pl.ds(d, PLANES)]
            bk = bk_ref[pl.ds(d, PLANES)]
            for c in range(3):
                mid = u(c, d, 0, 8)
                near = along_y(mid, ht[c, pl.ds(d + 2, PLANES)])
                coef = sh + bk if c == 1 else sh
                buf[core(c, d)] = buf[core(c, d)] + coef * second(mid, *near)
                if c == 1:
                    bb_ref[pl.ds(d, PLANES)] = first(*near)
            return carry

        lax.fori_loop(0, blocks, sideways, 0)

        await_halos(range(2))
        for lo in (0, 16):
            buf[par, 2, 0, lo : lo + 8, :] = buf[par, 2, 4, lo : lo + 8, :]
            buf[par, 2, 1, lo : lo + 8, :] = buf[par, 2, 3, lo : lo + 8, :]

        def prepare(b, carry):
            d = b * PLANES
            a = first(u(0, d, 0, 9), u(0, d, 0, 7), u(0, d, 0, 10), u(0, d, 0, 6))
            bb = bb_ref[pl.ds(d, PLANES)]
            e_ref[pl.ds(d + 2, PLANES)] = a + bb
            cc = cc_ref[pl.ds(d, PLANES)]
            s_ref[pl.ds(d, PLANES), 8:16, :] = bb + cc

            def mixed(comp, shift):
                return jnp.where(row3 < 4, u(comp, d, shift, 16), u(comp, d, shift, 0))

            s_halo = first(*along_y(mixed(1, 0), hx[pl.ds(d, PLANES)])) + first(
                mixed(2, 1), mixed(2, -1), mixed(2, 2), mixed(2, -2)
            )
            s_ref[pl.ds(d, PLANES), 0:8, :] = s_halo
            s_ref[pl.ds(d, PLANES), 16:24, :] = s_halo
            return carry

        lax.fori_loop(0, blocks, prepare, 0)
        e_ref[0] = e_ref[4]
        e_ref[1] = e_ref[3]

        def advance(b, carry):
            d = b * PLANES
            sh = sh_ref[pl.ds(d, PLANES)]
            bk = bk_ref[pl.ds(d, PLANES)]

            def h(c, shift):
                return ht[c, pl.ds(d + 2 + shift, PLANES)]

            def s(lo):
                return s_ref[pl.ds(d, PLANES), lo : lo + 8, :]

            def e(shift):
                return e_ref[pl.ds(d + 2 + shift, PLANES)]

            a = first(u(0, d, 0, 9), u(0, d, 0, 7), u(0, d, 0, 10), u(0, d, 0, 6))
            cc = cc_ref[pl.ds(d, PLANES)]
            c_halo = first(h(2, 1), h(2, -1), h(2, 2), h(2, -2))
            t_halo = ah[pl.ds(d, PLANES)] + c_halo
            for c in range(3):
                mid = u(c, d, 0, 8)
                along = second(mid, u(c, d, 0, 9), u(c, d, 0, 7), u(c, d, 0, 10), u(c, d, 0, 6))
                if c == 0:
                    cross = first(s(9), s(7), s(10), s(6))
                elif c == 1:
                    cross = first(*along_y(a + cc, t_halo))
                else:
                    cross = first(e(1), e(-1), e(2), e(-2))
                coef = sh + bk if c == 0 else sh
                buf[core(c, d)] = buf[core(c, d)] + (coef * along + bk * cross)
            return carry

        lax.fori_loop(0, blocks, advance, 0)
        for k in range(8):
            @pl.when(exists(*DIRECTIONS[k]))
            def _():
                copy_of(k, par).wait_send()
        surf_ref[lax.div(n, every)] = buf[new, :, 2, 8:16, :]
        return carry

    lax.fori_loop(0, steps, step, 0)
    f_ref[...] = buf[steps % 2, :, 2 : nz + 2, 8:16, :]


def run_grid(displacement, previous, shear_coef, bulk_coef):
    _, nz, cx, cy = displacement.shape
    vmem = pl.BlockSpec(memory_space=pltpu.VMEM)
    f32 = jnp.float32
    return pl.pallas_call(
        functools.partial(grid_kernel, COUPLINGS * EVERY, EVERY),
        out_shape=(
            jax.ShapeDtypeStruct(displacement.shape, f32),
            jax.ShapeDtypeStruct((COUPLINGS, 3, cx, cy), f32),
        ),
        in_specs=[vmem] * 4,
        out_specs=(vmem, vmem),
        scratch_shapes=[
            pltpu.VMEM((2, 3, nz + 4, cx + 16, cy), f32),
            pltpu.VMEM((2, 3, cx, cy), f32),
            pltpu.VMEM((2, 2, 3, cx + 16, cy), f32),
            pltpu.VMEM((3, nz + 4, cx, cy), f32),
            pltpu.VMEM((nz, cx, cy), f32),
            pltpu.VMEM((nz, cx, cy), f32),
            pltpu.VMEM((nz + 4, cx, cy), f32),
            pltpu.VMEM((nz, cx + 16, cy), f32),
            pltpu.VMEM((nz, cx, cy), f32),
            pltpu.VMEM((nz, cx, cy), f32),
            pltpu.SemaphoreType.DMA((2, 8)),
            pltpu.SemaphoreType.DMA((2, 8)),
        ],
        compiler_params=pltpu.CompilerParams(
            collective_id=0, has_side_effects=True, vmem_limit_bytes=32 * 1024 * 1024
        ),
    )(displacement, previous, shear_coef, bulk_coef)


def building_kernel(couplings, sub, m_ref, f_ref, t_ref, o_ref):
    block, rows, _ = m_ref.shape
    width = t_ref.shape[1]
    states = [jnp.zeros((rows, width), jnp.float32) for _ in range(block)]
    for moment in range(couplings):
        drives = []
        for i in range(block):
            drive = m_ref[i, :, 3 * moment : 3 * moment + 1] * f_ref[i, 0:1, :]
            drive = drive + m_ref[i, :, 3 * moment + 1 : 3 * moment + 2] * f_ref[i, 1:2, :]
            drive = drive + m_ref[i, :, 3 * moment + 2 : 3 * moment + 3] * f_ref[i, 2:3, :]
            drives.append(drive)
        for inner in range(sub):
            for i in range(block):
                if moment == 0 and inner == 0:
                    states[i] = drives[i]
                else:
                    states[i] = drives[i] + lax.dot_general(
                        states[i].astype(jnp.bfloat16), t_ref[i],
                        (((1,), (1,)), ((), ())), preferred_element_type=jnp.float32,
                    )
    for i in range(block):
        o_ref[:, CAP * i : CAP * (i + 1), :] = states[i].reshape(rows // CAP, CAP, width)


def run_buildings(motion, forcing, transition, start, kinds):
    rows, parts = motion.shape[1], motion.shape[2]
    width = transition.shape[1]
    first_block = start // ARCH_BLOCK
    return pl.pallas_call(
        functools.partial(building_kernel, COUPLINGS, SUB),
        grid=(kinds // ARCH_BLOCK,),
        out_shape=jax.ShapeDtypeStruct((rows // CAP, kinds * CAP, width), jnp.float32),
        in_specs=[
            pl.BlockSpec((ARCH_BLOCK, rows, parts), lambda i: (i + first_block, 0, 0)),
            pl.BlockSpec((ARCH_BLOCK, 3, width), lambda i: (i + first_block, 0, 0)),
            pl.BlockSpec((ARCH_BLOCK, width, width), lambda i: (i + first_block, 0, 0)),
        ],
        out_specs=pl.BlockSpec((rows // CAP, ARCH_BLOCK * CAP, width), lambda i: (0, i, 0)),
        cost_estimate=pl.CostEstimate(
            flops=2 * kinds * rows * width * width * COUPLINGS * SUB,
            bytes_accessed=2 * kinds * width * width + 4 * kinds * rows * width,
            transcendentals=0,
        ),
    )(motion, forcing, transition)


def per_device(
    displacement, previous, shear_coef, bulk_coef, cell_index, archetype_id, transition, forcing
):
    groups = lax.axis_size("slab") * lax.axis_size("gy")
    arch_local = transition.shape[0]
    width = transition.shape[1]
    slots_dev = arch_local * CAP
    count = cell_index.shape[0]
    kinds = archetype_id[:, 0]
    order = jnp.arange(count, dtype=jnp.int32)
    earlier = (kinds[:, None] == kinds[None, :]) & (order[None, :] < order[:, None])
    position = jnp.sum(earlier.astype(jnp.int32), axis=1)
    slot_index = kinds * CAP + position
    cells = displacement.shape[2] * displacement.shape[3] * lax.axis_size("gy")
    local_cell = cell_index - lax.axis_index("slab") * cells
    slots = jnp.arange(groups * slots_dev, dtype=jnp.int32)
    slot_cell = jnp.sum(
        jnp.where(slot_index[None, :] == slots[:, None], local_cell[None, :], 0), axis=1
    )

    field, surface = run_grid(displacement, previous, shear_coef, bulk_coef)

    parts = 3 * COUPLINGS
    surface = lax.all_gather(surface, "gy", axis=3, tiled=True)
    table = surface.reshape(parts, cells).T
    motion = jnp.take(table, slot_cell, axis=0, mode="clip")
    motion = motion.reshape(groups, slots_dev, parts).transpose(0, 2, 1)
    pushed = lax.all_to_all(motion, ("slab", "gy"), split_axis=0, concat_axis=0, tiled=True)
    pushed = pushed.reshape(groups, parts, arch_local, CAP).transpose(2, 0, 3, 1)
    pushed = pushed.reshape(arch_local, groups * CAP, parts)

    share = arch_local // CHUNKS
    pieces = []
    for chunk in range(CHUNKS):
        states = run_buildings(pushed, forcing, transition, chunk * share, share)
        returned = lax.all_to_all(
            states, ("slab", "gy"), split_axis=0, concat_axis=0, tiled=True
        )
        pieces.append(returned.reshape(groups * share * CAP, width))
    owner, kind = kinds // arch_local, kinds % arch_local
    chunk_of = kind // share
    home = chunk_of * (groups * share * CAP) + owner * (share * CAP)
    home = home + (kind - chunk_of * share) * CAP + position
    home_state = jnp.take(jnp.concatenate(pieces, axis=0), home, axis=0, mode="clip")
    return (field, home_state)


def solution(mesh):
    in_specs = (
        P(None, None, "slab", "gy"),
        P(None, None, "slab", "gy"),
        P(None, "slab", "gy"),
        P(None, "slab", "gy"),
        P(("slab", "gy")),
        P(("slab", "gy"), None),
        P(("slab", "gy"), None, None),
        P(("slab", "gy"), None, None),
    )
    out_specs = (P(None, None, "slab", "gy"), P(("slab", "gy"), None))
    return jax.shard_map(
        per_device, mesh=mesh, in_specs=in_specs, out_specs=out_specs, check_vma=False
    )
```
